32 devices in a mesh: dp: 1 (over z), ey: 4 (over y), ex: 8 (over x, core).
Axes of the slice: x: 4, y: 4, z: 1, core: 2. Of those that a mesh axis runs over, the one named last changes fastest.
The devices are a block of a 4x4x8 slice.
Arguments:
- x: bfloat16 [16384, 2048], P(('dp', 'ey', 'ex'))
- ids: int32 [16384, 6], P(('dp', 'ey', 'ex'))
- gates: float32 [16384, 6], P(('dp', 'ey', 'ex'))
- w1: bfloat16 [64, 2048, 1408], P(('ey', 'ex'))
- w3: bfloat16 [64, 2048, 1408], P(('ey', 'ex'))
- w2: bfloat16 [64, 1408, 2048], P(('ey', 'ex'))
Outputs:
- output: bfloat16 [16384, 2048], P(('dp', 'ey', 'ex'))
All inputs are finite; a program needn't handle non-finite values.
Results may differ from the reference program's by a relative error of at most 0.00601959.
Values are sent between devices in bfloat16 or wider.
A program may use at most 768 MiB of HBM per device.

```python
import jax
import jax.numpy as jnp
from jax import lax

H = 2048
F = 1408
E = 64
TOP = 6
NG = 1
TG = 1
T = 512
P = 32

EL = E // P
N = P * T
GN = max(NG, 8)
GT = TG + (GN // 2 - TG) * (1 // NG)
EG = E // GN
CAP = min(T, 2 * T * TOP // P)


def setup_inputs(seed: int = 0, part: int = 0) -> dict:
    kw1, kw3, kw2 = jax.random.split(jax.random.key(seed), 3)
    kb1, kb2 = jax.random.split(jax.random.fold_in(jax.random.key(seed), 7), 2)
    kpart = jax.random.fold_in(jax.random.key(seed + 1), part)
    kx, _, _, ka = jax.random.split(kpart, 4)
    kg, ke = jax.random.split(jax.random.fold_in(kpart, 7), 2)
    x = jax.random.normal(kx, (N, H), jnp.float32)
    group_bias = jax.random.randint(kb1, (GN,), 0, 2 ** 21, jnp.int32)
    bias_draw = jax.random.randint(kb2, (E,), 0, 2 ** 10, jnp.int32)
    expert_bias = (3 * bias_draw * bias_draw) >> 1
    group_draw = jax.random.randint(kg, (N, GN), 0, 2 ** 20, jnp.int32)
    group_score = (group_draw + group_bias[None, :]) * GN + jnp.arange(GN, dtype=jnp.int32)[None, :]
    gtop = lax.top_k(group_score, GT)[1]
    gmask = jnp.any(gtop[:, :, None] == jnp.arange(GN)[None, None, :], axis=1)
    emask = jnp.repeat(gmask, EG, axis=1).astype(jnp.int32)
    expert_draw = jax.random.randint(ke, (N, E), 0, 2 ** 20, jnp.int32)
    expert_score = (expert_draw + expert_bias[None, :] + (4 << 20) * emask) * E + jnp.arange(E, dtype=jnp.int32)[None, :]
    ids = lax.top_k(expert_score, TOP)[1].astype(jnp.int32)
    a = jax.random.uniform(ka, (N, TOP), jnp.float32, 0.5, 1.5)
    gates = 2.5 * a / jnp.sum(a, axis=1, keepdims=True)
    w1 = jax.random.normal(kw1, (E, H, F), jnp.float32) * H ** -0.5
    w3 = jax.random.normal(kw3, (E, H, F), jnp.float32) * H ** -0.5
    w2 = jax.random.normal(kw2, (E, F, H), jnp.float32) * F ** -0.5
    return {"x": x.astype(jnp.bfloat16), "ids": ids, "gates": gates,
            "w1": w1.astype(jnp.bfloat16), "w3": w3.astype(jnp.bfloat16),
            "w2": w2.astype(jnp.bfloat16)}


def keep_mask(ids):
    dev = ids // EL
    hit = jnp.any(dev[:, :, None] == jnp.arange(P)[None, None, :], axis=1)
    hit3 = hit.reshape(P, T, P)
    rank = jnp.cumsum(hit3.astype(jnp.int32), axis=1) - 1
    kept = (hit3 & (rank < CAP)).reshape(N, P)
    return jnp.take_along_axis(kept, dev, axis=1)


def reference(x, ids, gates, w1, w3, w2):
    wk = gates * keep_mask(ids).astype(jnp.float32)

    def body(acc, e):
        c = jnp.sum(jnp.where(ids == e, wk, 0.0), axis=1)
        a1 = jnp.dot(x, w1[e], preferred_element_type=jnp.float32)
        a3 = jnp.dot(x, w3[e], preferred_element_type=jnp.float32)
        h = (jax.nn.silu(a1) * a3).astype(jnp.bfloat16)
        o = jnp.dot(h, w2[e], preferred_element_type=jnp.float32).astype(jnp.bfloat16)
        return acc + c[:, None] * o.astype(jnp.float32), None

    acc, _ = lax.scan(body, jnp.zeros((N, H), jnp.float32), jnp.arange(E))
    return (x.astype(jnp.float32) + acc).astype(jnp.bfloat16)
```

```python
import functools

import jax
import jax.numpy as jnp
from jax import lax
from jax.experimental import pallas as pl
from jax.experimental.pallas import tpu as pltpu
from jax.sharding import Mesh
from jax.sharding import PartitionSpec as P

CAPF = 2
CORES = 2
PARTS = 2
BW = 256
TM = 512
MSIZES = (64, 128, 192, BW + 16)
AXES = ("ey", "x")


def _share_kernel(ny, nx, a_ref, b_ref, ao_ref, bo_ref, send_sem, recv_sem, own_sem):
    nr = ny * nx
    me = lax.axis_index("ey") * nx + lax.axis_index("x")

    def peer(k):
        d = lax.rem(me + k, nr)
        return {"ey": d // nx, "x": lax.rem(d, nx)}

    pairs = ((a_ref, ao_ref), (b_ref, bo_ref))
    barrier = pltpu.get_barrier_semaphore()
    for k in range(1, nr):
        pl.semaphore_signal(barrier, inc=1, device_id=peer(k))
    copies = [pltpu.make_async_copy(s, d.at[me], own_sem.at[i]) for i, (s, d) in enumerate(pairs)]
    for c in copies:
        c.start()
    pl.semaphore_wait(barrier, nr - 1)
    for k in range(1, nr):
        for i, (s, d) in enumerate(pairs):
            c = pltpu.make_async_remote_copy(
                src_ref=s, dst_ref=d.at[me], send_sem=send_sem.at[i, k],
                recv_sem=recv_sem.at[i, k], device_id=peer(k))
            c.start()
            copies.append(c)
    for c in copies:
        c.wait()


def _share(a, b, ny, nx):
    vm = pl.BlockSpec(memory_space=pltpu.VMEM)
    nr = ny * nx
    return pl.pallas_call(
        functools.partial(_share_kernel, ny, nx),
        out_shape=[jax.ShapeDtypeStruct((nr,) + v.shape, v.dtype) for v in (a, b)],
        in_specs=[vm, vm],
        out_specs=[vm, vm],
        scratch_shapes=[pltpu.SemaphoreType.DMA((2, nr)), pltpu.SemaphoreType.DMA((2, nr)),
                        pltpu.SemaphoreType.DMA((2,))],
        compiler_params=pltpu.CompilerParams(collective_id=0, has_side_effects=True),
        name="share",
    )(a, b)


def _ffn_kernel(nel, rreg, starts, posm, xg, *refs):
    ws, (o, xb, w1v, w3v, w2v, buf, hv, of, ob, xsem, wsem, osem) = refs[:6], refs[6:]
    ne = 2 * nel
    nblk = posm.shape[1]
    hd = xg.shape[1]
    f = w1v.shape[2]
    kr = hd // 128

    def rows_of(e):
        return starts[e, nblk]

    def weights(e, op):
        slot = lax.rem(e, 2)
        for half in range(2):
            @pl.when((e >= half * nel) & (e < (half + 1) * nel))
            def _(half=half):
                for i, v in enumerate((w1v, w3v, w2v)):
                    src = ws[half * 3 + i].at[e - half * nel]
                    getattr(pltpu.make_async_copy(src, v.at[slot], wsem.at[slot, i]), op)()

    def ocopy(row, slot):
        return pltpu.make_async_copy(
            ob.at[slot], o.at[pl.ds(pl.multiple_of(row * kr, 16), TM * kr)], osem.at[slot])

    def process(e, tile, g):
        ws_ = lax.rem(e, 2)

        @pl.when(tile == 0)
        def _():
            weights(e, "wait")

        def up(n, _):
            col = pl.ds(pl.multiple_of(n * 128, 128), 128)
            w = jnp.concatenate([w1v[ws_, :, col], w3v[ws_, :, col]], axis=1)
            a = jnp.dot(buf[0:TM], w, preferred_element_type=jnp.float32)
            a1 = a[:, :128]
            hv[:, col] = (a1 * jax.nn.sigmoid(a1) * a[:, 128:]).astype(hv.dtype)
            return 0

        lax.fori_loop(0, f // 128, up, 0)

        def down(n, _):
            r = jnp.dot(hv[...], w2v[ws_, :, pl.ds(pl.multiple_of(n * 256, 256), 256)],
                        preferred_element_type=jnp.float32)
            for i in range(2):
                of[pl.ds(n * 2 + i, TM, stride=kr), :] = r[:, i * 128:(i + 1) * 128]
            return 0

        lax.fori_loop(0, hd // 256, down, 0)
        slot = lax.rem(g, 2)

        @pl.when(g >= 2)
        def _():
            ocopy(0, slot).wait()

        def narrow(n, _):
            r = pl.ds(pl.multiple_of(n * 512, 512), 512)
            ob[slot, r] = of[r].astype(ob.dtype)
            return 0

        lax.fori_loop(0, TM * kr // 512, narrow, 0)
        ocopy(e * rreg + tile * TM, slot).start()

    def expert(e, g0):
        def some(b):
            return starts[e, b + 1] > starts[e, b]

        def xcopy(b, op):
            slot = lax.rem(b, 3)

            @pl.when(some(b))
            def _():
                getattr(pltpu.make_async_copy(
                    xg.at[pl.ds(pl.multiple_of(b * BW, BW), BW)], xb.at[slot], xsem.at[slot]), op)()

        @pl.when((e + 1 < ne) & (rows_of(jnp.minimum(e + 1, ne - 1)) > 0))
        def _():
            weights(e + 1, "start")

        xcopy(0, "start")
        xcopy(1, "start")

        def body(b, carry):
            tile, g = carry

            @pl.when(b + 2 < nblk)
            def _():
                xcopy(jnp.minimum(b + 2, nblk - 1), "start")

            xcopy(b, "wait")
            slot = lax.rem(b, 3)
            s = starts[e, b]
            end = starts[e, b + 1]
            off = s - tile * TM
            al = pl.multiple_of((off // 16) * 16, 16)
            need = end - tile * TM - al

            def append(m):
                rel = posm[e, b] - (tile * TM + al)
                rows = lax.broadcasted_iota(jnp.int32, (m, BW), 0)
                oh = jnp.where(rows == rel, 1.0, 0.0).astype(buf.dtype)
                old = lax.broadcasted_iota(jnp.int32, (16, 512), 0) < off - al
                for n in range(hd // 512):
                    c = slice(n * 512, (n + 1) * 512)
                    r = jnp.dot(oh, xb[slot, :, c], preferred_element_type=jnp.float32)
                    head = pl.ds(al, 16)
                    buf[head, c] = jnp.where(
                        old, buf[head, c].astype(jnp.float32), r[:16]).astype(buf.dtype)
                    buf[pl.ds(al + 16, m - 16), c] = r[16:].astype(buf.dtype)

            lo = 0
            for m in MSIZES:
                @pl.when((end > s) & (need > lo) & (need <= m))
                def _(m=m):
                    append(m)
                lo = m

            full = end - tile * TM >= TM

            @pl.when(full)
            def _():
                process(e, tile, g)
                buf[0:BW + 16] = buf[TM:TM + BW + 16]

            inc = full.astype(jnp.int32)
            return tile + inc, g + inc

        tile, g = lax.fori_loop(0, nblk, body, (jnp.int32(0), g0))
        more = rows_of(e) > tile * TM

        @pl.when(more)
        def _():
            process(e, tile, g)

        return g + more.astype(jnp.int32)

    @pl.when(rows_of(0) > 0)
    def _():
        weights(jnp.int32(0), "start")

    g = lax.fori_loop(0, ne, expert, jnp.int32(0))
    for back in (2, 1):
        @pl.when(g >= back)
        def _(back=back):
            ocopy(0, lax.rem(g - back + 2, 2)).wait()


def _ffn(starts, posm, xg, ws, rreg):
    n, hd = xg.shape
    nel, _, f = ws[0].shape
    kr = hd // 128
    anyspec = pl.BlockSpec(memory_space=pl.ANY)
    return pl.pallas_call(
        functools.partial(_ffn_kernel, nel, rreg),
        out_shape=jax.ShapeDtypeStruct(((2 * nel * rreg + BW) * kr, 128), jnp.bfloat16),
        in_specs=[pl.BlockSpec(memory_space=pltpu.SMEM), pl.BlockSpec(memory_space=pltpu.VMEM)]
        + [anyspec] * 7,
        out_specs=anyspec,
        scratch_shapes=[
            pltpu.VMEM((3, BW, hd), jnp.bfloat16),
            pltpu.VMEM((2, hd, f), jnp.bfloat16),
            pltpu.VMEM((2, hd, f), jnp.bfloat16),
            pltpu.VMEM((2, f, hd), jnp.bfloat16),
            pltpu.VMEM((TM + BW + 16, hd), jnp.bfloat16),
            pltpu.VMEM((TM, f), jnp.bfloat16),
            pltpu.VMEM((TM * kr, 128), jnp.float32),
            pltpu.VMEM((2, TM * kr, 128), jnp.bfloat16),
            pltpu.SemaphoreType.DMA((3,)),
            pltpu.SemaphoreType.DMA((2, 3)),
            pltpu.SemaphoreType.DMA((2,)),
        ],
        compiler_params=pltpu.CompilerParams(vmem_limit_bytes=60 * 1024 * 1024),
        cost_estimate=pl.CostEstimate(flops=6 * rreg * 2 * hd * f, transcendentals=0,
                                      bytes_accessed=n * hd * 2),
        name="ffn",
    )(starts, posm, xg, *ws)


def _spread_kernel(ne, rreg, starts, idx, wgt, o, y, win, wsem):
    b = pl.program_id(0)
    nblk = pl.num_programs(0)
    kr = y.shape[0] // BW

    def window(b, op):
        slot = lax.rem(b, 2)
        for e in range(ne):
            @pl.when(starts[e, b + 1] > starts[e, b])
            def _(e=e):
                src = o.at[pl.ds(pl.multiple_of((e * rreg + starts[e, b]) * kr, 16), BW * kr)]
                getattr(pltpu.make_async_copy(
                    src, win.at[slot, pl.ds(e * BW * kr, BW * kr)], wsem.at[slot, e]), op)()

    @pl.when(b == 0)
    def _():
        for s in range(2):
            win[s, pl.ds(ne * BW * kr, kr)] = jnp.zeros((kr, 128), win.dtype)
        window(b, "start")

    @pl.when(b + 1 < nblk)
    def _():
        window(jnp.minimum(b + 1, nblk - 1), "start")

    window(b, "wait")
    slot = lax.rem(b, 2)

    def body(n, _):
        acc = None
        for e in range(ne):
            r = pl.ds(pl.multiple_of(idx[0, e, n], 16), kr)
            v = wgt[0, e, n] * win[slot, r].astype(jnp.float32)
            acc = v if acc is None else acc + v
        y[pl.ds(pl.multiple_of(n * kr, 16), kr)] = acc
        return 0

    lax.fori_loop(0, BW, body, 0, unroll=8)


def _spread(starts, idx, wgt, o, rreg, kr):
    ne = starts.shape[0]
    nblk = idx.shape[0]
    sm = lambda *a: pl.BlockSpec(*a, memory_space=pltpu.SMEM)
    return pl.pallas_call(
        functools.partial(_spread_kernel, ne, rreg),
        grid=(nblk,),
        out_shape=jax.ShapeDtypeStruct((nblk * BW * kr, 128), jnp.float32),
        in_specs=[sm(), sm((1, ne, BW), lambda b: (b, 0, 0)), sm((1, ne, BW), lambda b: (b, 0, 0)),
                  pl.BlockSpec(memory_space=pl.ANY)],
        out_specs=pl.BlockSpec((BW * kr, 128), lambda b: (b, 0)),
        scratch_shapes=[pltpu.VMEM((2, (ne * BW + 1) * kr, 128), jnp.bfloat16),
                        pltpu.SemaphoreType.DMA((2, ne))],
        compiler_params=pltpu.CompilerParams(vmem_limit_bytes=40 * 1024 * 1024),
        cost_estimate=pl.CostEstimate(flops=nblk * BW * kr * 128 * 2000, transcendentals=0,
                                      bytes_accessed=nblk * BW * kr * 1024),
        name="spread",
    )(starts, idx, wgt, o)


def _rank(a, tri):
    return jnp.dot(a.astype(jnp.bfloat16), tri.astype(jnp.bfloat16),
                   preferred_element_type=jnp.float32).astype(jnp.int32)


def _before(n):
    return jnp.arange(n)[:, None] < jnp.arange(n)[None, :]


def solution(mesh):
    ndp, ny, nex = (mesh.shape[a] for a in ("dp", "ey", "ex"))
    nx = nex // CORES
    nr = ny * nx
    grid = Mesh(mesh.devices.reshape(ndp, ny, nx, CORES), ("dp", "ey", "x", "core"))
    tok = P(("dp", "ey", "x", "core"), None)
    wsp = P(("ey", "x", "core"), None, None)

    def local(x, ids, gates, w1, w3, w2):
        t, hd = x.shape
        top = ids.shape[1]
        el = w1.shape[0]
        ne = CORES * el
        kr = hd // 128
        cap = min(t, CAPF * t * top // (nr * CORES))
        tc = t // PARTS
        nblk = nr * tc // BW
        me = (lax.axis_index("ey") * nx + lax.axis_index("x")) * CORES + lax.axis_index("core")
        mate = me + 1 - 2 * lax.axis_index("core")

        xg = [lax.all_gather(x[c * tc:(c + 1) * tc], AXES, axis=0, tiled=True)
              for c in range(PARTS)]
        swap = [(i, CORES - 1 - i) for i in range(CORES)]
        ws = [w1, w3, w2] + [lax.ppermute(w, "core", swap) for w in (w1, w3, w2)]

        pad = ((0, 8 - top), (0, 0))
        ida, gta = _share(jnp.pad(ids.T, pad, constant_values=-1), jnp.pad(gates.T, pad), ny, nx)
        sel, gat = [], []
        for q in (me, mate):
            hit = jnp.any((ida >= q * el) & (ida < (q + 1) * el), axis=1)
            kept = hit & (_rank(hit, _before(t)) < cap)
            for e in range(el):
                m = ida == q * el + e
                sel.append(jnp.any(m, axis=1) & kept)
                gat.append(jnp.sum(jnp.where(m, gta, 0.0), axis=1))
        sel, gat = jnp.stack(sel), jnp.stack(gat)

        rreg = -(-nr * min(tc, cap) // TM) * TM
        ys = []
        for c in range(PARTS):
            cs = slice(c * tc, (c + 1) * tc)
            se = sel[:, :, cs]
            n = jnp.sum(se.astype(jnp.int32), axis=2)
            base = jnp.sum(jnp.where(_before(nr)[None], n[:, :, None], 0), axis=1)
            pos = _rank(se.reshape(ne * nr, tc), _before(tc)).reshape(ne, nr, tc) + base[:, :, None]
            pos = pos.reshape(ne, nblk, BW)
            se = se.reshape(ne, nblk, BW)
            st = pos[:, :, 0]
            starts = jnp.concatenate([st, jnp.sum(n, axis=1)[:, None]], axis=1)
            o = _ffn(starts, jnp.where(se, pos, -1)[:, :, None], xg[c], ws, rreg)
            off = (jnp.arange(ne) * BW)[:, None, None]
            idx = jnp.where(se, pos - st[:, :, None] + off, ne * BW) * kr
            wgt = jnp.where(se, gat[:, :, cs].reshape(ne, nblk, BW), 0.0)
            d = _spread(starts, idx.transpose(1, 0, 2), wgt.transpose(1, 0, 2), o, rreg, kr)
            ys.append(lax.psum_scatter(d, AXES, scatter_dimension=0, tiled=True))
        y = jnp.concatenate(ys).reshape(t, hd)
        return (x.astype(jnp.float32) + y).astype(x.dtype)

    return jax.shard_map(local, mesh=grid, in_specs=(tok, tok, tok, wsp, wsp, wsp),
                         out_specs=tok, check_vma=False)
```

```python
import functools

import jax
import jax.numpy as jnp
from jax import lax
from jax.experimental import pallas as pl
from jax.experimental.pallas import tpu as pltpu
from jax.sharding import Mesh
from jax.sharding import PartitionSpec as P

CAPF = 2
CORES = 2
CUTS = (2, 2, 4)
BW = 256
TM = 512
UPW = 256
DNW = 512
APW = 1024
SPW = 512
WSIZES = (64, 144, 208, BW + 16)
XS = 5
MSIZES = (128, BW + 16)
AXES = ("ey", "x")


def _share_kernel(ny, nx, a_ref, b_ref, ao_ref, bo_ref, send_sem, recv_sem, own_sem):
    nr = ny * nx
    me = lax.axis_index("ey") * nx + lax.axis_index("x")

    def peer(k):
        d = lax.rem(me + k, nr)
        return {"ey": d // nx, "x": lax.rem(d, nx)}

    pairs = ((a_ref, ao_ref), (b_ref, bo_ref))
    barrier = pltpu.get_barrier_semaphore()
    for k in range(1, nr):
        pl.semaphore_signal(barrier, inc=1, device_id=peer(k))
    copies = [pltpu.make_async_copy(s, d.at[me], own_sem.at[i]) for i, (s, d) in enumerate(pairs)]
    for c in copies:
        c.start()
    pl.semaphore_wait(barrier, nr - 1)
    for k in range(1, nr):
        for i, (s, d) in enumerate(pairs):
            c = pltpu.make_async_remote_copy(
                src_ref=s, dst_ref=d.at[me], send_sem=send_sem.at[i, k],
                recv_sem=recv_sem.at[i, k], device_id=peer(k))
            c.start()
            copies.append(c)
    for c in copies:
        c.wait()


def _share(a, b, ny, nx):
    vm = pl.BlockSpec(memory_space=pltpu.VMEM)
    nr = ny * nx
    return pl.pallas_call(
        functools.partial(_share_kernel, ny, nx),
        out_shape=[jax.ShapeDtypeStruct((nr,) + v.shape, v.dtype) for v in (a, b)],
        in_specs=[vm, vm],
        out_specs=[vm, vm],
        scratch_shapes=[pltpu.SemaphoreType.DMA((2, nr)), pltpu.SemaphoreType.DMA((2, nr)),
                        pltpu.SemaphoreType.DMA((2,))],
        compiler_params=pltpu.CompilerParams(collective_id=0, has_side_effects=True),
        name="share",
    )(a, b)


def _ffn_kernel(nel, rreg, starts, posm, xg, *refs):
    ws, (o, xb, w1v, w3v, w2v, buf, hv, ob, xsem, wsem, osem) = refs[:6], refs[6:]
    ne = 2 * nel
    nblk = posm.shape[1]
    hd = xg.shape[1]
    f = w1v.shape[2]

    def rows_of(e):
        return starts[e, nblk]

    def weights(e, op, which=(0, 1, 2)):
        slot = lax.rem(e, 2)
        for half in range(2):
            @pl.when((e >= half * nel) & (e < (half + 1) * nel))
            def _(half=half):
                for i in which:
                    v = (w1v, w3v, w2v)[i]
                    src = ws[half * 3 + i].at[e - half * nel]
                    getattr(pltpu.make_async_copy(src, v.at[slot], wsem.at[slot, i]), op)()

    def ocopy(row, slot):
        return pltpu.make_async_copy(
            ob.at[slot], o.at[pl.ds(pl.multiple_of(row, 16), TM)], osem.at[slot])

    def process(e, tile, g, m):
        ws_ = lax.rem(e, 2)

        @pl.when(tile == 0)
        def _():
            weights(e, "wait", (0, 1))

        def up(col, width):
            w = jnp.concatenate([w1v[ws_, :, col], w3v[ws_, :, col]], axis=1)
            a = jnp.dot(buf[0:m], w, preferred_element_type=jnp.float32)
            a1 = a[:, :width]
            hv[0:m, col] = (a1 * jax.nn.sigmoid(a1) * a[:, width:]).astype(hv.dtype)

        def upn(n, _):
            up(pl.ds(pl.multiple_of(n * UPW, UPW), UPW), UPW)
            return 0

        lax.fori_loop(0, f // UPW, upn, 0)
        if f % UPW:
            up(pl.ds(f - f % UPW, f % UPW), f % UPW)

        @pl.when(tile == 0)
        def _():
            weights(e, "wait", (2,))

        slot = lax.rem(g, 2)

        @pl.when(g >= 2)
        def _():
            ocopy(0, slot).wait()

        def down(n, _):
            col = pl.ds(pl.multiple_of(n * DNW, DNW), DNW)
            r = jnp.dot(hv[0:m], w2v[ws_, :, col], preferred_element_type=jnp.float32)
            ob[slot, 0:m, col] = r.astype(ob.dtype)
            return 0

        lax.fori_loop(0, hd // DNW, down, 0)
        ocopy(e * rreg + tile * TM, slot).start()

    def expert(e, g0):
        def xcopy(b, op):
            slot = lax.rem(b, XS)

            @pl.when(starts[e, b + 1] > starts[e, b])
            def _():
                getattr(pltpu.make_async_copy(
                    xg.at[pl.ds(pl.multiple_of(b * BW, BW), BW)], xb.at[slot], xsem.at[slot]), op)()

        for b in range(XS - 1):
            xcopy(b, "start")

        @pl.when((e + 1 < ne) & (rows_of(jnp.minimum(e + 1, ne - 1)) > 0))
        def _():
            weights(e + 1, "start")

        def body(b, carry):
            tile, g = carry

            @pl.when(b + XS - 1 < nblk)
            def _():
                xcopy(jnp.minimum(b + XS - 1, nblk - 1), "start")

            xcopy(b, "wait")
            slot = lax.rem(b, XS)
            s = starts[e, b]
            end = starts[e, b + 1]
            off = s - tile * TM
            al = pl.multiple_of((off // 16) * 16, 16)
            need = end - tile * TM - al

            def append(m):
                rel = posm[e, b] - (tile * TM + al)
                rows = lax.broadcasted_iota(jnp.int32, (m, BW), 0)
                oh = jnp.where(rows == rel, 1.0, 0.0).astype(buf.dtype)
                old = lax.broadcasted_iota(jnp.int32, (16, APW), 0) < off - al
                for n in range(hd // APW):
                    c = slice(n * APW, (n + 1) * APW)
                    r = jnp.dot(oh, xb[slot, :, c], preferred_element_type=jnp.float32)
                    head = pl.ds(al, 16)
                    buf[head, c] = jnp.where(
                        old, buf[head, c].astype(jnp.float32), r[:16]).astype(buf.dtype)
                    buf[pl.ds(al + 16, m - 16), c] = r[16:].astype(buf.dtype)

            lo = 0
            for m in MSIZES:
                @pl.when((end > s) & (need > lo) & (need <= m))
                def _(m=m):
                    append(m)
                lo = m

            left = end - tile * TM
            todo = jnp.where(b == nblk - 1, left + TM - 1, left) // TM

            def run(i, _):
                few = left - i * TM <= TM // 2
                pl.when(few)(lambda: process(e, tile + i, g + i, TM // 2))
                pl.when(jnp.logical_not(few))(lambda: process(e, tile + i, g + i, TM))
                buf[0:BW + 16] = buf[TM:TM + BW + 16]
                return 0

            lax.fori_loop(0, todo, run, 0)
            return tile + todo, g + todo

        return lax.fori_loop(0, nblk, body, (jnp.int32(0), g0))[1]

    @pl.when(rows_of(0) > 0)
    def _():
        weights(jnp.int32(0), "start")

    buf[...] = jnp.zeros_like(buf)
    g = lax.fori_loop(0, ne, expert, jnp.int32(0))
    for back in (2, 1):
        @pl.when(g >= back)
        def _(back=back):
            ocopy(0, lax.rem(g - back + 2, 2)).wait()


def _ffn(starts, posm, xg, ws, rreg):
    n, hd = xg.shape
    nel, _, f = ws[0].shape
    anyspec = pl.BlockSpec(memory_space=pl.ANY)
    return pl.pallas_call(
        functools.partial(_ffn_kernel, nel, rreg),
        out_shape=jax.ShapeDtypeStruct((2 * nel * rreg + BW + 16, hd), jnp.bfloat16),
        in_specs=[pl.BlockSpec(memory_space=pltpu.SMEM), pl.BlockSpec(memory_space=pltpu.VMEM)]
        + [anyspec] * 7,
        out_specs=anyspec,
        scratch_shapes=[
            pltpu.VMEM((XS, BW, hd), jnp.bfloat16),
            pltpu.VMEM((2, hd, f), jnp.bfloat16),
            pltpu.VMEM((2, hd, f), jnp.bfloat16),
            pltpu.VMEM((2, f, hd), jnp.bfloat16),
            pltpu.VMEM((TM + BW + 16, hd), jnp.bfloat16),
            pltpu.VMEM((TM, f), jnp.bfloat16),
            pltpu.VMEM((2, TM, hd), jnp.bfloat16),
            pltpu.SemaphoreType.DMA((XS,)),
            pltpu.SemaphoreType.DMA((2, 3)),
            pltpu.SemaphoreType.DMA((2,)),
        ],
        compiler_params=pltpu.CompilerParams(vmem_limit_bytes=62 * 1024 * 1024),
        cost_estimate=pl.CostEstimate(flops=6 * rreg * 2 * hd * f, transcendentals=0,
                                      bytes_accessed=n * hd * 2),
        name="ffn",
    )(starts, posm, xg, *ws)


def _spread_kernel(ne, rreg, starts, tab, o, y, win, cols, wsem):
    b = pl.program_id(0)
    nblk = pl.num_programs(0)
    hd = y.shape[1]

    def base(e, b):
        return pl.multiple_of((starts[e, b] // 16) * 16, 16)

    def classes(e, b, sizes, fn):
        need = starts[e, b + 1] - base(e, b)
        some = starts[e, b + 1] > starts[e, b]
        lo = 0
        for k in sizes:
            pl.when(some & (need > lo) & (need <= k))(functools.partial(fn, k))
            lo = k

    def window(b, op):
        slot = lax.rem(b, 2)

        def one(e, _):
            def copy(k):
                src = o.at[pl.ds(pl.multiple_of(e * rreg + base(e, b), 16), k)]
                getattr(pltpu.make_async_copy(
                    src, win.at[slot, e, pl.ds(0, k)], wsem.at[slot, e]), op)()

            classes(e, b, WSIZES, copy)
            return 0

        lax.fori_loop(0, ne, one, 0)

    @pl.when(b == 0)
    def _():
        win[...] = jnp.zeros_like(win)
        window(b, "start")

    @pl.when(b + 1 < nblk)
    def _():
        window(jnp.minimum(b + 1, nblk - 1), "start")

    window(b, "wait")
    slot = lax.rem(b, 2)
    for e in range(ne):
        cols[e] = jnp.transpose(tab[0, e])
    wide = False
    for e in range(ne):
        lo = base(e, b)
        stop = starts[e, nblk] - lo
        wide = (starts[e, b + 1] - lo > BW) | wide

        @pl.when((starts[e, b + 1] > starts[e, b]) & (stop < BW + 16))
        def _(e=e, stop=stop):
            def clear(i, _):
                r = pl.ds(pl.multiple_of(i * 16, 16), 16)
                keep = lax.broadcasted_iota(jnp.int32, (16, hd), 0) + i * 16 < stop
                win[slot, e, r] = jnp.where(
                    keep, win[slot, e, r].astype(jnp.float32), 0.0).astype(win.dtype)
                return 0

            lax.fori_loop(0, BW // 16 + 1, clear, 0)

    def pick(e, k):
        at = cols[e, :, 0:1].astype(jnp.int32) - base(e, b)
        lane = lax.broadcasted_iota(jnp.int32, (BW, k), 1)
        return jnp.where(lane == at, 1.0, 0.0).astype(win.dtype)

    @pl.when(jnp.logical_not(wide))
    def _():
        oh = [pick(e, BW) for e in range(ne)]
        for n in range(hd // SPW):
            c = slice(n * SPW, (n + 1) * SPW)
            acc = 0.0
            for e in range(ne):
                acc = acc + cols[e, :, 1:2] * jnp.dot(
                    oh[e], win[slot, e, :BW, c], preferred_element_type=jnp.float32)
            y[:, c] = acc

    @pl.when(wide)
    def _():
        y[...] = jnp.zeros_like(y)

        def one(e, _):
            for n in range(hd // 1024):
                c = slice(n * 1024, (n + 1) * 1024)
                y[:, c] = y[:, c] + cols[e, :, 1:2] * jnp.dot(
                    pick(e, BW + 16), win[slot, e, :, c], preferred_element_type=jnp.float32)
            return 0

        lax.fori_loop(0, ne, one, 0)


def _spread(starts, tab, o, rreg):
    nblk, ne = tab.shape[:2]
    hd = o.shape[1]
    return pl.pallas_call(
        functools.partial(_spread_kernel, ne, rreg),
        grid=(nblk,),
        out_shape=jax.ShapeDtypeStruct((nblk * BW, hd), jnp.float32),
        in_specs=[pl.BlockSpec(memory_space=pltpu.SMEM),
                  pl.BlockSpec((1,) + tab.shape[1:], lambda b: (b, 0, 0, 0)),
                  pl.BlockSpec(memory_space=pl.ANY)],
        out_specs=pl.BlockSpec((BW, hd), lambda b: (b, 0)),
        scratch_shapes=[pltpu.VMEM((2, ne, BW + 16, hd), jnp.bfloat16),
                        pltpu.VMEM((ne, BW, tab.shape[2]), jnp.float32),
                        pltpu.SemaphoreType.DMA((2, ne))],
        compiler_params=pltpu.CompilerParams(vmem_limit_bytes=40 * 1024 * 1024),
        cost_estimate=pl.CostEstimate(flops=nblk * BW * hd * 2000, transcendentals=0,
                                      bytes_accessed=nblk * BW * hd * 8),
        name="spread",
    )(starts, tab, o)


def _rank(a, tri):
    return jnp.dot(a.astype(jnp.bfloat16), tri.astype(jnp.bfloat16),
                   preferred_element_type=jnp.float32).astype(jnp.int32)


def _before(n):
    return jnp.arange(n)[:, None] < jnp.arange(n)[None, :]


def solution(mesh):
    ndp, ny, nex = (mesh.shape[a] for a in ("dp", "ey", "ex"))
    nx = nex // CORES
    nr = ny * nx
    grid = Mesh(mesh.devices.reshape(ndp, ny, nx, CORES), ("dp", "ey", "x", "core"))
    tok = P(("dp", "ey", "x", "core"), None)
    wsp = P(("ey", "x", "core"), None, None)

    def local(x, ids, gates, w1, w3, w2):
        t, hd = x.shape
        top = ids.shape[1]
        el = w1.shape[0]
        ne = CORES * el
        cap = min(t, CAPF * t * top // (nr * CORES))
        cuts = [0]
        for part in CUTS:
            cuts.append(cuts[-1] + t * part // sum(CUTS))
        spans = list(zip(cuts[:-1], cuts[1:]))
        me = (lax.axis_index("ey") * nx + lax.axis_index("x")) * CORES + lax.axis_index("core")
        mate = me + 1 - 2 * lax.axis_index("core")

        xg = [lax.all_gather(x[i:j], AXES, axis=0, tiled=True) for i, j in spans]
        swap = [(i, CORES - 1 - i) for i in range(CORES)]
        ws = [w1, w3, w2] + [lax.ppermute(w, "core", swap) for w in (w1, w3, w2)]

        pad = ((0, 8 - top), (0, 0))
        ida, gta = _share(jnp.pad(ids.T, pad, constant_values=-1), jnp.pad(gates.T, pad), ny, nx)
        sel, gat = [], []
        for q in (me, mate):
            hit = jnp.any((ida >= q * el) & (ida < (q + 1) * el), axis=1)
            kept = hit & (_rank(hit, _before(t)) < cap)
            for e in range(el):
                m = ida == q * el + e
                sel.append(jnp.any(m, axis=1) & kept)
                gat.append(jnp.sum(jnp.where(m, gta, 0.0), axis=1))
        sel, gat = jnp.stack(sel), jnp.stack(gat)

        ys = []
        for c, (i, j) in enumerate(spans):
            tc = j - i
            nblk = nr * tc // BW
            rreg = -(-nr * min(tc, cap) // TM) * TM
            se = sel[:, :, i:j]
            n = jnp.sum(se.astype(jnp.int32), axis=2)
            base = jnp.sum(jnp.where(_before(nr)[None], n[:, :, None], 0), axis=1)
            pos = _rank(se.reshape(ne * nr, tc), _before(tc)).reshape(ne, nr, tc) + base[:, :, None]
            pos = pos.reshape(ne, nblk, BW)
            se = se.reshape(ne, nblk, BW)
            starts = jnp.concatenate([pos[:, :, 0], jnp.sum(n, axis=1)[:, None]], axis=1)
            at = jnp.where(se, pos, -1)
            o = _ffn(starts, at[:, :, None], xg[c], ws, rreg)
            wgt = jnp.where(se, gat[:, :, i:j].reshape(ne, nblk, BW), 0.0)
            tab = jnp.stack([at.astype(jnp.float32), wgt], axis=2).transpose(1, 0, 2, 3)
            tab = jnp.pad(tab, ((0, 0), (0, 0), (0, 6), (0, 0)))
            d = _spread(starts, tab, o, rreg)
            ys.append(lax.psum_scatter(d, AXES, scatter_dimension=0, tiled=True))
        return (x.astype(jnp.float32) + jnp.concatenate(ys)).astype(x.dtype)

    return jax.shard_map(local, mesh=grid, in_specs=(tok, tok, tok, wsp, wsp, wsp),
                         out_specs=tok, check_vma=False)
```
